32 devices in a mesh: seq: 16 (over z, y, core), tp: 2 (over x).
Axes of the slice: x: 2, y: 2, z: 4, core: 2. Of those that a mesh axis runs over, the one named last changes fastest.
Arguments:
- video_query: bfloat16 [2, 8192, 3072], P(None, 'seq', 'tp'), may hold values from -2048 to 2048
- text_states: bfloat16 [2, 256, 4096], P(None, 'seq'), may hold values from -24 to 24
- key_weight: bfloat16 [4096, 3072], P(None, 'tp'), may hold values from -1 to 1
- value_weight: bfloat16 [4096, 3072], P(None, 'tp'), may hold values from -0.09375 to 0.09375
- text_lengths: int32 [2], replicated, may hold values from 64 to 256, as said below
- output_grad: bfloat16 [2, 8192, 3072], P(None, 'seq', 'tp'), may hold values from -6 to 6
Outputs:
- attended: bfloat16 [2, 8192, 3072], P(None, 'seq', 'tp')
- query_grad: bfloat16 [2, 8192, 3072], P(None, 'seq', 'tp')
- key_weight_grad: float32 [4096, 3072], P('seq', 'tp')
- value_weight_grad: float32 [4096, 3072], P('seq', 'tp')
The draws below stay inside these ranges and needn't reach their ends.
Inputs may be any that keep to these rules, and one draw needn't show every extreme that they name: Keys of sample b at text positions from text_lengths[b] on are masked; one sample has all 256 text tokens.
All inputs are finite; a program needn't handle non-finite values.
Results may differ from the reference program's by a relative error of at most 0.012.
The reference program's roundings to bfloat16 on the way (of `key_states`, `value_states`, `probs_low` and `dscore`) count: a program that leaves them out, or rounds other values in their place, can miss the bound.
Values may be sent and summed in bfloat16 or wider, within the bound.
A program may use at most 128 MiB of HBM per device.

```python
import math
import jax
import jax.numpy as jnp
from jax import lax

DT = 4096
HEADS = 24
HEAD = 128
TEXT = 256
SAMPLES = 2
VIDEO = 8192


def column_rise(ratio):
    position = jnp.arange(DT, dtype=jnp.float32) / max(DT - 1, 1)
    rising = 1.0 + (ratio - 1.0) * position
    return rising / jnp.sqrt(jnp.mean(rising * rising))


def shared_draw(key):
    text_key = jax.random.fold_in(key, 101)
    weight_key = jax.random.fold_in(key, 102)
    states = jax.random.truncated_normal(text_key, -6.0, 6.0, (SAMPLES, TEXT, DT), jnp.float32)
    states = states * column_rise(3.0)[None, None, :]
    weight = jax.random.truncated_normal(weight_key, -6.0, 6.0, (DT, HEADS * HEAD), jnp.float32) / math.sqrt(DT)
    return (states.astype(jnp.bfloat16), weight.astype(jnp.bfloat16))


def draw_text_states(key, part):
    return shared_draw(key)[0]


def draw_key_weight(key, part):
    return shared_draw(key)[1]


def draw_text_lengths(key, part):
    length_key = jax.random.fold_in(key, 104)
    others = jax.random.randint(jax.random.fold_in(length_key, 1), (SAMPLES,), TEXT // 4, TEXT, jnp.int32)
    chosen = jax.random.randint(jax.random.fold_in(length_key, 2), (), 0, SAMPLES, jnp.int32)
    return jnp.where(jnp.arange(SAMPLES, dtype=jnp.int32) == chosen, jnp.int32(TEXT), others).astype(jnp.int32)


def draw_video_query(key, part):
    query_key = jax.random.fold_in(key, 103)
    feature_count = HEADS * HEAD
    base = jax.random.truncated_normal(query_key, -6.0, 6.0, (SAMPLES, VIDEO, feature_count), jnp.float32)
    return base.astype(jnp.bfloat16)


def steps_of(key, dims, split, smallest, largest):
    factor_of, own = 1.0, jax.random.fold_in(key, 6)
    for dim, blocks in split:
        heights = jnp.exp(jax.random.uniform(jax.random.fold_in(own, dim), (blocks,), jnp.float32, smallest / len(split), largest / len(split)))
        factor_of = factor_of * jnp.repeat(heights, dims[dim] // blocks).reshape([-1 if axis == dim else 1 for axis in range(len(dims))])
    return factor_of


def noise(stream_key, shape, scale, limit, shards=(), held_as=jnp.bfloat16):
    drawn = jax.random.normal(stream_key, shape, jnp.float32) * scale
    if len(shards) > 0:
        drawn = steps_of(stream_key, shape, shards, -0.22, 0.18) * drawn
    return jnp.clip(drawn, min=-limit, max=limit).astype(held_as)


def setup_inputs(seed: int = 0) -> dict:
    key_of = jax.random.split(jax.random.key(seed), 7)
    return {
        "video_query": draw_video_query(jax.random.fold_in(key_of[6], 71), 0),
        "text_states": draw_text_states(jax.random.fold_in(key_of[6], 71), 0),
        "key_weight": draw_key_weight(jax.random.fold_in(key_of[6], 71), 0),
        "value_weight": noise(key_of[3], (DT, HEADS * HEAD), DT ** -0.5, 0.09375, ((1, 2),)),
        "text_lengths": draw_text_lengths(jax.random.fold_in(key_of[6], 71), 0),
        "output_grad": noise(key_of[5], (SAMPLES, VIDEO, HEADS * HEAD), 1.0, 6.0, ((1, 16), (2, 2))),
    }


def reference(video_query, text_states, key_weight, value_weight, text_lengths, output_grad):
    samples = video_query.shape[0]
    key_states = lax.optimization_barrier(jnp.dot(text_states, key_weight, preferred_element_type=jnp.float32).astype(jnp.bfloat16))
    value_states = lax.optimization_barrier(jnp.dot(text_states, value_weight, preferred_element_type=jnp.float32).astype(jnp.bfloat16))
    scaling = 1.0 / math.sqrt(HEAD)
    allowed = jnp.arange(TEXT)[None, None, :] < text_lengths[:, None, None]

    def split_heads(tensor, length):
        return tensor.reshape(samples, length, HEADS, HEAD).transpose(2, 0, 1, 3)

    def per_head(operands):
        query_head, key_head, value_head, grad_head = [piece.astype(jnp.float32) for piece in operands]
        scores = jnp.einsum('bte,ble->btl', query_head, key_head) * scaling
        scores = jnp.where(allowed, scores, -1e+30)
        highest = lax.optimization_barrier(jnp.max(scores, axis=-1, keepdims=True))
        weights = jnp.exp(scores - highest)
        probs = weights / lax.optimization_barrier(jnp.sum(weights, axis=-1, keepdims=True))
        probs_low = lax.optimization_barrier(probs.astype(jnp.bfloat16)).astype(jnp.float32)
        attended = jnp.einsum('btl,ble->bte', probs_low, value_head).astype(jnp.bfloat16)
        dprob = jnp.einsum('bte,ble->btl', grad_head, value_head)
        delta = lax.optimization_barrier(jnp.sum(probs * dprob, axis=-1, keepdims=True))
        dscore = lax.optimization_barrier((probs * (dprob - delta) * scaling).astype(jnp.bfloat16)).astype(jnp.float32)
        query_grad = jnp.einsum('btl,ble->bte', dscore, key_head).astype(jnp.bfloat16)
        key_grad = jnp.einsum('btl,bte->ble', dscore, query_head)
        value_grad = jnp.einsum('btl,bte->ble', probs_low, grad_head)
        return (attended, query_grad, key_grad, value_grad)
    results = lax.map(per_head, (split_heads(video_query, VIDEO), split_heads(key_states, TEXT), split_heads(value_states, TEXT), split_heads(output_grad, VIDEO)))

    def merge_heads(tensor):
        return tensor.transpose(1, 2, 0, 3).reshape(samples, tensor.shape[2], HEADS * HEAD)
    attended = merge_heads(results[0])
    query_grad = merge_heads(results[1])
    key_grad = merge_heads(results[2])
    value_grad = merge_heads(results[3])
    text_wide = text_states.astype(jnp.float32)
    key_raw = jnp.einsum('bld,ble->de', text_wide, key_grad, precision=lax.Precision.HIGHEST)
    value_raw = jnp.einsum('bld,ble->de', text_wide, value_grad, precision=lax.Precision.HIGHEST)
    squares = jnp.sum(key_raw * key_raw) + jnp.sum(value_raw * value_raw)
    spread = jnp.sqrt(squares / (2.0 * DT * HEADS * HEAD) + 1e-06)
    factor = 1.0 / jnp.maximum(spread, 1.0)
    return (attended, query_grad, key_raw * factor, value_raw * factor)
```

```python
import functools
import math

import jax
import jax.numpy as jnp
from jax import lax
from jax.experimental import pallas as pl
from jax.experimental.pallas import tpu as pltpu
from jax.sharding import PartitionSpec as P

HEAD = 128
MESH = pl.DeviceIdType.MESH
NEG = -1e30


def rem(a, b):
    return lax.rem(a, b)


class Place:
    def __init__(self, n):
        self.C = 2
        self.Y = 2
        self.Z = n // 4
        self.n = n
        me = lax.axis_index("seq")
        self.me = me
        self.tp = lax.axis_index("tp")
        self.c = rem(me, 2)
        self.y = rem(me // 2, 2)
        self.z = me // 4

    def dev(self, z, y, c):
        return ((z * self.Y + y) * self.C + c, self.tp)

    def core_peer(self):
        return self.dev(self.z, self.y, 1 - self.c)

    def y_peer(self):
        return self.dev(self.z, 1 - self.y, self.c)

    def z_ahead(self, d):
        return rem(self.z + d, self.Z)

    def z_behind(self, d):
        return rem(self.z + self.Z - d, self.Z)

    def z_peer(self, d):
        return self.dev(self.z_ahead(d), self.y, self.c)


def rcopy(src, dst, ssem, rsem, dev):
    return pltpu.make_async_remote_copy(
        src_ref=src, dst_ref=dst, send_sem=ssem, recv_sem=rsem, device_id=dev, device_id_type=MESH
    )


def greet(devices):
    barrier = pltpu.get_barrier_semaphore()
    for d in devices:
        pl.semaphore_signal(barrier, inc=1, device_id=d, device_id_type=MESH)
    pl.semaphore_wait(barrier, len(devices))


class Gather:
    def __init__(self, pos, block, own, ss, rs):
        self.pos, self.block, self.own, self.ss, self.rs = pos, block, own, ss, rs
        self.sent = []

    def copy(self, src, z, y, c, k, dev):
        d = rcopy(src, self.block(z, y, c), self.ss(k), self.rs(k), dev)
        return d

    def go(self, src, z, y, c, k, dev):
        d = self.copy(src, z, y, c, k, dev)
        d.start()
        self.sent.append(d)

    def start(self):
        p = self.pos
        for d in range(p.Z - 1, 0, -1):
            self.go(self.own, p.z, p.y, p.c, d - 1, p.z_peer(d))
        self.go(self.own, p.z, p.y, p.c, p.Z - 1, p.y_peer())
        self.go(self.own, p.z, p.y, p.c, 2 * p.Z - 1, p.core_peer())

    def arrive_z(self, d):
        p = self.pos
        self.sent[p.Z - 1 - d].wait_recv()
        zz = p.z_behind(d)
        self.go(self.block(zz, p.y, p.c), zz, p.y, p.c, p.Z - 1 + d, p.y_peer())
        self.go(self.block(zz, p.y, p.c), zz, p.y, p.c, 2 * p.Z - 1 + d, p.core_peer())

    def arrive_y(self, d):
        p = self.pos
        zz = p.z_behind(d)
        src = self.block(zz, 1 - p.y, p.c)
        rcopy(src, src, self.ss(p.Z - 1 + d), self.rs(p.Z - 1 + d), p.y_peer()).wait_recv()
        self.go(src, zz, 1 - p.y, p.c, 3 * p.Z - 1 + d, p.core_peer())

    def finish(self):
        p = self.pos
        for d in range(2 * p.Z):
            k = 2 * p.Z - 1 + d
            src = self.own
            rcopy(src, src, self.ss(k), self.rs(k), p.core_peer()).wait_recv()
        for d in self.sent:
            d.wait_send()


def gather_kernel(n, k_loc, v_loc, text, k_out, v_out, cols, gs, gr, ts, tr):
    p = Place(n)
    width = cols.shape[-1]
    greet([(rem(p.me + d, n), p.tp) for d in range(1, n)])
    flows = []
    for i, (loc, out) in enumerate(((k_loc, k_out), (v_loc, v_out))):
        f = Gather(
            p,
            lambda z, y, c, out=out: out.at[z, y, c],
            loc,
            lambda k, i=i: gs.at[i, k],
            lambda k, i=i: gr.at[i, k],
        )
        f.start()
        flows.append(f)
    direct = []
    for d in range(1, n):
        to = rem(p.me + d, n)
        start = pl.multiple_of(to * width, 128)
        cp = rcopy(
            text.at[:, :, pl.ds(start, width)], cols.at[p.me], ts.at[d - 1], tr.at[d - 1], (to, p.tp)
        )
        cp.start()
        direct.append(cp)
    k_out[p.z, p.y, p.c] = k_loc[...]
    v_out[p.z, p.y, p.c] = v_loc[...]
    cols[p.me] = text[:, :, pl.ds(pl.multiple_of(p.me * width, 128), width)]
    for d in range(1, p.Z):
        for f in flows:
            f.arrive_z(d)
    for d in range(p.Z):
        for f in flows:
            f.arrive_y(d)
    for f in flows:
        f.finish()
    for cp in direct:
        cp.wait()


def reduce_kernel(n, gk, gv, tk, tv, s1k, s1v, r1k, r1v, s2k, s2v, r2k, r2v, r3k, r3v, own_k, own_v,
                  ss, rs, gs, gr):
    p = Place(n)
    Z = p.Z
    width = gk.shape[-1]
    cut = 2 if width % 256 == 0 else 1
    step = width // cut
    chunks = []
    for h in range(cut):
        for refs in ((gk, tk, s1k, r1k, s2k, r2k, r3k, own_k), (gv, tv, s1v, r1v, s2v, r2v, r3v, own_v)):
            chunks.append((refs, pl.ds(h * step, step)))
    greet([p.core_peer(), p.y_peer()] + [p.z_peer(d) for d in range(1, Z)])
    f32, low = jnp.float32, jnp.bfloat16
    first = []
    for i, ((g, t, s1, r1, s2, r2, r3, own), w) in enumerate(chunks):
        cp = rcopy(
            g.at[:, :, 1 - p.c, :, :, w], r1.at[:, :, :, :, w], ss.at[i, 0], rs.at[i, 0], p.core_peer()
        )
        cp.start()
        first.append(cp)
    second = []
    for i, ((g, t, s1, r1, s2, r2, r3, own), w) in enumerate(chunks):
        first[i].wait_recv()
        for yy in (1 - p.y, p.y):
            s1[:, yy, :, :, w] = (
                g[:, yy, p.c, :, :, w].astype(f32) + r1[:, yy, :, :, w].astype(f32)
            ).astype(low)
            if yy is not p.y:
                cp = rcopy(
                    s1.at[:, 1 - p.y, :, :, w], r2.at[:, :, :, w], ss.at[i, 1], rs.at[i, 1], p.y_peer()
                )
                cp.start()
                second.append(cp)
    third = []
    for i, ((g, t, s1, r1, s2, r2, r3, own), w) in enumerate(chunks):
        second[i].wait_recv()
        mine = []
        for d in range(Z - 1, 0, -1):
            zz = p.z_ahead(d)
            s2[zz, :, :, w] = (
                s1[zz, p.y, :, :, w].astype(f32) + r2[zz, :, :, w].astype(f32)
            ).astype(low)
            cp = rcopy(
                s2.at[zz, :, :, w], r3.at[d - 1, :, :, w], ss.at[i, 1 + d], rs.at[i, 1 + d], p.z_peer(d)
            )
            cp.start()
            mine.append(cp)
        third.append(mine)
    flows = []
    for i, ((g, t, s1, r1, s2, r2, r3, own), w) in enumerate(chunks):
        total = s1[p.z, p.y, :, :, w].astype(f32) + r2[p.z, :, :, w].astype(f32)
        for cp in third[i]:
            cp.wait_recv()
        for d in range(1, Z):
            total = total + r3[d - 1, :, :, w].astype(f32)
        own[:, :, w] = total.astype(low)
        f = Gather(
            p,
            lambda z, y, c, t=t, w=w: t.at[z, y, c, :, :, w],
            own.at[:, :, w],
            lambda k, i=i: gs.at[i, k],
            lambda k, i=i: gr.at[i, k],
        )
        f.start()
        t[p.z, p.y, p.c, :, :, w] = total.astype(low)
        flows.append(f)
    for f in flows:
        for d in range(1, Z):
            f.arrive_z(d)
    for f in flows:
        for d in range(Z):
            f.arrive_y(d)
    for f in flows:
        f.finish()
    for cp in first + second + [c for m in third for c in m]:
        cp.wait_send()


def scalar_kernel(n, m, x, out, ss, rs):
    me, tp = lax.axis_index("seq"), lax.axis_index("tp")
    flat = me * m + tp
    peers = []
    for d in range(1, n * m):
        to = rem(flat + d, n * m)
        peers.append((to // m, rem(to, m)))
    greet(peers)
    copies = []
    for d, dev in enumerate(peers):
        cp = rcopy(x, out.at[flat], ss.at[d], rs.at[d], dev)
        cp.start()
        copies.append(cp)
    out[flat] = x[...]
    for cp in copies:
        cp.wait()


def flat_rows(x):
    n, r, e = x.shape
    if r % 16 == 0:
        return x.reshape(n * r, e)
    return x.astype(jnp.float32).reshape(n * r, e).astype(x.dtype)


def attention_kernel(scaling, lengths, q_ref, k_ref, v_ref, g_ref, a_ref, qg_ref, kg_ref, vg_ref):
    f32, low = jnp.float32, jnp.bfloat16
    length = lengths[pl.program_id(0)]
    q, g = q_ref[0], g_ref[0]
    k, v = flat_rows(k_ref[:, 0]), flat_rows(v_ref[:, 0])
    n, _, r, e = k_ref.shape
    last = (((1,), (1,)), ((), ()))
    head = (((0,), (0,)), ((), ()))
    s = lax.dot_general(k, q, last, preferred_element_type=f32)
    dp = lax.dot_general(v, g, last, preferred_element_type=f32)
    row = lax.broadcasted_iota(jnp.int32, s.shape, 0)
    s = jnp.where(row < length, s, NEG)
    top = jnp.max(s, axis=0, keepdims=True)
    w = jnp.exp2((s - top) * (scaling * math.log2(math.e)))
    inv = 1.0 / jnp.sum(w, axis=0, keepdims=True)
    probs = w * inv
    probs_low = probs.astype(low)
    delta = jnp.sum(probs * dp, axis=0, keepdims=True)
    ds = (probs * (dp - delta) * scaling).astype(low)
    a_ref[0] = lax.dot_general(v, probs_low, head, preferred_element_type=f32).astype(low).T
    qg_ref[0] = lax.dot_general(k, ds, head, preferred_element_type=f32).astype(low).T
    kg = jnp.dot(ds, q, preferred_element_type=f32)
    vg = jnp.dot(probs_low, g, preferred_element_type=f32)
    kg_ref[:, 0] = kg.reshape(n, r, e).astype(low)
    vg_ref[:, 0] = vg.reshape(n, r, e).astype(low)


VM = pl.BlockSpec(memory_space=pltpu.VMEM)
BIG = 60 * 1024 * 1024


def per_device(n, m, all_features, video_query, text_states, key_weight, value_weight, text_lengths, output_grad):
    samples, rows, features = video_query.shape
    _, r, depth = text_states.shape
    heads = features // HEAD
    low, f32 = jnp.bfloat16, jnp.float32
    Z, Y, C = n // 4, 2, 2
    dma = pltpu.SemaphoreType.DMA
    k_loc = jnp.dot(text_states, key_weight, preferred_element_type=f32).astype(low)
    v_loc = jnp.dot(text_states, value_weight, preferred_element_type=f32).astype(low)
    spread6 = jax.ShapeDtypeStruct((Z, Y, C, samples, r, features), low)
    k_full, v_full, cols = pl.pallas_call(
        functools.partial(gather_kernel, n),
        out_shape=(spread6, spread6, jax.ShapeDtypeStruct((n, samples, r, depth // n), low)),
        in_specs=[VM] * 3,
        out_specs=(VM,) * 3,
        scratch_shapes=[dma((2, 4 * Z - 1)), dma((2, 4 * Z - 1)), dma((n - 1,)), dma((n - 1,))],
        compiler_params=pltpu.CompilerParams(
            collective_id=0, has_side_effects=True, vmem_limit_bytes=BIG
        ),
        name="gather_kv",
    )(k_loc, v_loc, text_states)
    text_spec = pl.BlockSpec((n, 1, r, HEAD), lambda b, h, s: (0, b, 0, h))
    video_spec = pl.BlockSpec((1, rows, HEAD), lambda b, h, s: (b, 0, h))
    video_out = jax.ShapeDtypeStruct(video_query.shape, low)
    text_out = jax.ShapeDtypeStruct((n, samples, r, features), low)
    attended, query_grad, kg, vg = pl.pallas_call(
        functools.partial(attention_kernel, 1.0 / math.sqrt(HEAD)),
        out_shape=(video_out, video_out, text_out, text_out),
        grid_spec=pltpu.PrefetchScalarGridSpec(
            num_scalar_prefetch=1,
            grid=(samples, heads),
            in_specs=[video_spec, text_spec, text_spec, video_spec],
            out_specs=(video_spec, video_spec, text_spec, text_spec),
        ),
        compiler_params=pltpu.CompilerParams(vmem_limit_bytes=32 * 1024 * 1024),
        name="attention",
    )(
        text_lengths,
        video_query,
        k_full.reshape(n, samples, r, features),
        v_full.reshape(n, samples, r, features),
        output_grad,
    )
    six = (Z, Y, C, samples, r, features)
    five = (Z, Y, samples, r, features)
    four = (Z, samples, r, features)
    vmem = pltpu.VMEM
    cuts = 2 * (2 if features % 256 == 0 else 1)
    tk, tv = pl.pallas_call(
        functools.partial(reduce_kernel, n),
        out_shape=(spread6, spread6),
        in_specs=[VM] * 2,
        out_specs=(VM,) * 2,
        scratch_shapes=[
            vmem(five, low), vmem(five, low), vmem(five, low), vmem(five, low),
            vmem(four, low), vmem(four, low), vmem(four, low), vmem(four, low),
            vmem((Z - 1,) + four[1:], low), vmem((Z - 1,) + four[1:], low),
            vmem(four[1:], low), vmem(four[1:], low),
            dma((cuts, Z + 1)), dma((cuts, Z + 1)),
            dma((cuts, 4 * Z - 1)), dma((cuts, 4 * Z - 1)),
        ],
        compiler_params=pltpu.CompilerParams(
            collective_id=1, has_side_effects=True, vmem_limit_bytes=BIG
        ),
        name="reduce_grads",
    )(kg.reshape(six), vg.reshape(six))
    cols = cols.reshape(n * samples * r, depth // n)
    over = (((0,), (0,)), ((), ()))
    key_raw = lax.dot_general(
        cols, tk.reshape(n * samples * r, features), over, preferred_element_type=f32
    )
    value_raw = lax.dot_general(
        cols, tv.reshape(n * samples * r, features), over, preferred_element_type=f32
    )
    squares = jnp.sum(key_raw * key_raw) + jnp.sum(value_raw * value_raw)
    parts = pl.pallas_call(
        functools.partial(scalar_kernel, n, m),
        out_shape=jax.ShapeDtypeStruct((n * m, 8, 128), f32),
        in_specs=[VM],
        out_specs=VM,
        scratch_shapes=[dma((n * m - 1,)), dma((n * m - 1,))],
        compiler_params=pltpu.CompilerParams(collective_id=2, has_side_effects=True),
        name="scalar_sum",
    )(jnp.broadcast_to(squares, (8, 128)))
    overall = jnp.sum(parts[:, 0, 0])
    spread = jnp.sqrt(overall / (2.0 * depth * all_features) + 1e-06)
    factor = 1.0 / jnp.maximum(spread, 1.0)
    return attended, query_grad, key_raw * factor, value_raw * factor


def solution(mesh):
    n, m = mesh.shape["seq"], mesh.shape["tp"]
    in_specs = (
        P(None, "seq", "tp"),
        P(None, "seq", None),
        P(None, "tp"),
        P(None, "tp"),
        P(),
        P(None, "seq", "tp"),
    )
    out_specs = (P(None, "seq", "tp"), P(None, "seq", "tp"), P("seq", "tp"), P("seq", "tp"))

    def step(*args):
        body = functools.partial(per_device, n, m, args[0].shape[2])
        return jax.shard_map(
            body, mesh=mesh, in_specs=in_specs, out_specs=out_specs, check_vma=False
        )(*args)

    return step
```

```python
import functools
import math

import jax
import jax.numpy as jnp
from jax import lax
from jax.experimental import pallas as pl
from jax.experimental.pallas import tpu as pltpu
from jax.sharding import PartitionSpec as P

HEAD = 128
MESH = pl.DeviceIdType.MESH
NEG = -1e30


def rem(a, b):
    return lax.rem(a, b)


class Place:
    def __init__(self, n):
        self.C = 2
        self.Y = 2
        self.Z = n // 4
        self.n = n
        me = lax.axis_index("seq")
        self.me = me
        self.tp = lax.axis_index("tp")
        self.c = rem(me, 2)
        self.y = rem(me // 2, 2)
        self.z = me // 4

    def dev(self, z, y, c):
        return ((z * self.Y + y) * self.C + c, self.tp)

    def core_peer(self):
        return self.dev(self.z, self.y, 1 - self.c)

    def y_peer(self):
        return self.dev(self.z, 1 - self.y, self.c)

    def z_ahead(self, d):
        return rem(self.z + d, self.Z)

    def z_behind(self, d):
        return rem(self.z + self.Z - d, self.Z)

    def z_peer(self, d):
        return self.dev(self.z_ahead(d), self.y, self.c)


def rcopy(src, dst, ssem, rsem, dev):
    return pltpu.make_async_remote_copy(
        src_ref=src, dst_ref=dst, send_sem=ssem, recv_sem=rsem, device_id=dev, device_id_type=MESH
    )


def greet(devices):
    barrier = pltpu.get_barrier_semaphore()
    for d in devices:
        pl.semaphore_signal(barrier, inc=1, device_id=d, device_id_type=MESH)
    pl.semaphore_wait(barrier, len(devices))


class Gather:
    def __init__(self, pos, block, own, ss, rs):
        self.pos, self.block, self.own, self.ss, self.rs = pos, block, own, ss, rs
        self.sent = []

    def copy(self, src, z, y, c, k, dev):
        d = rcopy(src, self.block(z, y, c), self.ss(k), self.rs(k), dev)
        return d

    def go(self, src, z, y, c, k, dev):
        d = self.copy(src, z, y, c, k, dev)
        d.start()
        self.sent.append(d)

    def start(self):
        p = self.pos
        for d in range(p.Z - 1, 0, -1):
            self.go(self.own, p.z, p.y, p.c, d - 1, p.z_peer(d))
        self.go(self.own, p.z, p.y, p.c, p.Z - 1, p.y_peer())
        self.go(self.own, p.z, p.y, p.c, 2 * p.Z - 1, p.core_peer())

    def arrive_z(self, d):
        p = self.pos
        self.sent[p.Z - 1 - d].wait_recv()
        zz = p.z_behind(d)
        self.go(self.block(zz, p.y, p.c), zz, p.y, p.c, p.Z - 1 + d, p.y_peer())
        self.go(self.block(zz, p.y, p.c), zz, p.y, p.c, 2 * p.Z - 1 + d, p.core_peer())

    def arrive_y(self, d):
        p = self.pos
        zz = p.z_behind(d)
        src = self.block(zz, 1 - p.y, p.c)
        rcopy(src, src, self.ss(p.Z - 1 + d), self.rs(p.Z - 1 + d), p.y_peer()).wait_recv()
        self.go(src, zz, 1 - p.y, p.c, 3 * p.Z - 1 + d, p.core_peer())

    def arrive_core(self):
        p = self.pos
        for d in range(2 * p.Z):
            k = 2 * p.Z - 1 + d
            src = self.own
            rcopy(src, src, self.ss(k), self.rs(k), p.core_peer()).wait_recv()

    def drain(self):
        for d in self.sent:
            d.wait_send()


def flat_rows(x):
    e = x.shape[-1]
    if x.shape[-2] % 16 == 0:
        return x.reshape(-1, e)
    return x.astype(jnp.float32).reshape(-1, e).astype(x.dtype)


def attend(scaling, length, q, g, k, v):
    f32, low = jnp.float32, jnp.bfloat16
    last = (((1,), (1,)), ((), ()))
    head = (((0,), (0,)), ((), ()))
    s = lax.dot_general(k, q, last, preferred_element_type=f32)
    dp = lax.dot_general(v, g, last, preferred_element_type=f32)
    row = lax.broadcasted_iota(jnp.int32, s.shape, 0)
    s = jnp.where(row < length, s, NEG)
    top = jnp.max(s, axis=0, keepdims=True)
    w = jnp.exp2((s - top) * (scaling * math.log2(math.e)))
    inv = 1.0 / jnp.sum(w, axis=0, keepdims=True)
    probs = w * inv
    probs_low = probs.astype(low)
    delta = jnp.sum(probs * dp, axis=0, keepdims=True)
    ds = (probs * (dp - delta) * scaling).astype(low)
    attended = lax.dot_general(v, probs_low, head, preferred_element_type=f32).astype(low).T
    query_grad = lax.dot_general(k, ds, head, preferred_element_type=f32).astype(low).T
    key_grad = jnp.dot(ds, q, preferred_element_type=f32)
    value_grad = jnp.dot(probs_low, g, preferred_element_type=f32)
    return attended, query_grad, key_grad, value_grad


def layer_kernel(n, m, groups, scaling, lengths, kv_loc, text, q_hbm, g_hbm, a_hbm, qg_hbm, raw, parts,
                 q, g, a, qg, kv, grads, s1, r1, s2, r2, r3, own, total, cols, cols_t, mine,
                 local, ks, kr, ts, tr, ss, rs, gs, gr, ps, pr):
    f32, low = jnp.float32, jnp.bfloat16
    p = Place(n)
    Z, Y, C = p.Z, p.Y, p.C
    samples, _, features = q.shape
    r = text.shape[1]
    width = cols.shape[-1]
    wide = features // groups
    heads = wide // HEAD
    part = [pl.ds(i * wide, wide) for i in range(groups)]
    loads = [
        pltpu.make_async_copy(q_hbm, q, local.at[0]),
        pltpu.make_async_copy(g_hbm, g, local.at[1]),
    ]
    for cp in loads:
        cp.start()
    flat = p.me * m + p.tp
    peers = []
    for d in range(1, n * m):
        to = rem(flat + d, n * m)
        peers.append((to // m, rem(to, m)))
    greet(peers)

    inward = []
    for i, w in enumerate(part):
        f = Gather(
            p,
            lambda z, y, c, w=w: kv.at[z, y, c, :, :, :, w],
            kv_loc.at[:, :, :, w],
            lambda k, i=i: ks.at[i, k],
            lambda k, i=i: kr.at[i, k],
        )
        f.start()
        inward.append(f)
    direct = []
    for d in range(1, n):
        to = rem(p.me + d, n)
        start = pl.multiple_of(to * width, 128)
        cp = rcopy(
            text.at[:, :, pl.ds(start, width)], cols.at[p.me], ts.at[d - 1], tr.at[d - 1], (to, p.tp)
        )
        cp.start()
        direct.append(cp)
    kv[p.z, p.y, p.c] = kv_loc[...]
    cols[p.me] = text[:, :, pl.ds(pl.multiple_of(p.me * width, 128), width)]

    def in_z(i):
        for d in range(1, Z):
            inward[i].arrive_z(d)

    def in_y(i):
        for d in range(Z):
            inward[i].arrive_y(d)

    def unit(i, b):
        length = lengths[b]

        def one(h, carry):
            w = pl.ds(pl.multiple_of((i * heads + h) * HEAD, HEAD), HEAD)
            k = flat_rows(kv[:, :, :, 0, b, :, w])
            v = flat_rows(kv[:, :, :, 1, b, :, w])
            att, q_grad, k_grad, v_grad = attend(scaling, length, q[b, :, w], g[b, :, w], k, v)
            a[b, :, w] = att
            qg[b, :, w] = q_grad
            grads[:, :, :, 0, b, :, w] = k_grad.reshape(Z, Y, C, r, HEAD).astype(low)
            grads[:, :, :, 1, b, :, w] = v_grad.reshape(Z, Y, C, r, HEAD).astype(low)
            return carry

        lax.fori_loop(0, heads, one, 0)

    sends, stores, outward = [], [], {}
    hold = {}

    def core_send(i):
        w = part[i]
        cp = rcopy(
            grads.at[:, :, 1 - p.c, :, :, :, w], r1.at[:, :, :, :, :, w], ss.at[i, 0], rs.at[i, 0],
            p.core_peer(),
        )
        cp.start()
        sends.append(cp)
        hold[i, 0] = cp
        for src, dst, k in ((a, a_hbm, 0), (qg, qg_hbm, 1)):
            st = pltpu.make_async_copy(src.at[:, :, w], dst.at[:, :, w], local.at[2 + 2 * i + k])
            st.start()
            stores.append(st)

    def core_sum(i):
        w = part[i]
        hold[i, 0].wait_recv()
        for far in (True, False):
            yy = 1 - p.y if far else p.y
            s1[:, yy, :, :, :, w] = (
                grads[:, yy, p.c, :, :, :, w].astype(f32) + r1[:, yy, :, :, :, w].astype(f32)
            ).astype(low)
            if far:
                cp = rcopy(
                    s1.at[:, yy, :, :, :, w], r2.at[:, :, :, :, w], ss.at[i, 1], rs.at[i, 1], p.y_peer()
                )
                cp.start()
                sends.append(cp)
                hold[i, 1] = cp

    def y_sum(i):
        w = part[i]
        hold[i, 1].wait_recv()
        for d in range(Z - 1, 0, -1):
            zz = p.z_ahead(d)
            s2[zz, :, :, :, w] = (
                s1[zz, p.y, :, :, :, w].astype(f32) + r2[zz, :, :, :, w].astype(f32)
            ).astype(low)
            cp = rcopy(
                s2.at[zz, :, :, :, w], r3.at[d - 1, :, :, :, w], ss.at[i, 1 + d], rs.at[i, 1 + d],
                p.z_peer(d),
            )
            cp.start()
            sends.append(cp)
            hold[i, 1 + d] = cp

    def z_sum(i):
        w = part[i]
        x = s1[p.z, p.y, :, :, :, w].astype(f32) + r2[p.z, :, :, :, w].astype(f32)
        for d in range(1, Z):
            hold[i, 1 + d].wait_recv()
            x = x + r3[d - 1, :, :, :, w].astype(f32)
        own[:, :, :, w] = x.astype(low)
        f = Gather(
            p,
            lambda z, y, c: total.at[z, y, c, :, :, :, w],
            own.at[:, :, :, w],
            lambda k: gs.at[i, k],
            lambda k: gr.at[i, k],
        )
        f.start()
        total[p.z, p.y, p.c, :, :, :, w] = x.astype(low)
        outward[i] = f

    def out_z(i):
        for d in range(1, Z):
            outward[i].arrive_z(d)

    def out_y(i):
        for d in range(Z):
            outward[i].arrive_y(d)

    squares = []

    def out_core(i):
        if i == 0:
            for cp in direct:
                cp.wait_recv()
            cols_t[...] = flat_rows(cols[...]).T
        outward[i].arrive_core()
        for kind in range(2):
            x = flat_rows(total[:, :, :, kind, :, :, part[i]])
            y = jnp.dot(cols_t[...], x, preferred_element_type=f32)
            raw[kind, :, part[i]] = y
            squares.append(jnp.sum((y * y).reshape(-1, 8, wide), axis=0))

    stages = (core_sum, y_sum, z_sum, out_z, out_y, out_core)
    pending = {}

    def turn():
        for i in sorted(pending):
            stages[pending[i]](i)
            pending[i] += 1
            if pending[i] == len(stages):
                del pending[i]

    in_z(0)
    in_y(0)
    if groups > 1:
        in_z(1)
    inward[0].arrive_core()
    for cp in loads:
        cp.wait()
    for i in range(groups):
        for b in range(samples):
            unit(i, b)
            if b == 0:
                if i + 1 < groups:
                    in_y(i + 1)
                if i + 2 < groups:
                    in_z(i + 2)
                turn()
        core_send(i)
        if i + 1 < groups:
            inward[i + 1].arrive_core()
        turn()
        pending[i] = 0
    while pending:
        turn()
    acc = squares[0]
    for x in squares[1:]:
        acc = acc + x
    mine[...] = jnp.broadcast_to(jnp.sum(acc, keepdims=True), mine.shape)
    last = []
    for d, dev in enumerate(peers):
        cp = rcopy(mine, parts.at[flat], ps.at[d], pr.at[d], dev)
        cp.start()
        last.append(cp)
    parts[flat] = mine[...]
    for st in stores:
        st.wait()
    for f in inward:
        f.drain()
    for i in sorted(outward):
        outward[i].drain()
    for cp in direct + sends:
        cp.wait_send()
    for cp in last:
        cp.wait()


VM = pl.BlockSpec(memory_space=pltpu.VMEM)
ANY = pl.BlockSpec(memory_space=pl.ANY)
BIG = 58 * 1024 * 1024


def per_device(n, m, all_features, video_query, text_states, key_weight, value_weight, text_lengths, output_grad):
    samples, rows, features = video_query.shape
    _, r, depth = text_states.shape
    heads = features // HEAD
    groups = 4 if heads % 4 == 0 else (3 if heads % 3 == 0 else 1)
    low, f32 = jnp.bfloat16, jnp.float32
    Z, Y, C = n // 4, 2, 2
    dma, vmem = pltpu.SemaphoreType.DMA, pltpu.VMEM
    k_loc = jnp.dot(text_states, key_weight, preferred_element_type=f32).astype(low)
    v_loc = jnp.dot(text_states, value_weight, preferred_element_type=f32).astype(low)
    kv_loc = jnp.stack((k_loc, v_loc))
    block = (2, samples, r, features)
    full = vmem((Z, Y, C) + block, low)
    half = vmem((Z, Y) + block, low)
    quarter = vmem((Z,) + block, low)
    video = vmem(video_query.shape, low)
    video_out = jax.ShapeDtypeStruct(video_query.shape, low)
    g_sems = (groups, 4 * Z - 1)
    attended, query_grad, raw, parts = pl.pallas_call(
        functools.partial(layer_kernel, n, m, groups, 1.0 / math.sqrt(HEAD)),
        out_shape=(
            video_out,
            video_out,
            jax.ShapeDtypeStruct((2, depth // n, features), f32),
            jax.ShapeDtypeStruct((n * m, 8, 128), f32),
        ),
        in_specs=[pl.BlockSpec(memory_space=pltpu.SMEM), VM, VM, ANY, ANY],
        out_specs=(ANY, ANY, VM, VM),
        scratch_shapes=[
            video, video, video, video,
            full, full, half, half, quarter, quarter, vmem((Z - 1,) + block, low), vmem(block, low), full,
            vmem((n, samples, r, depth // n), low), vmem((depth // n, n * samples * r), low),
            vmem((8, 128), f32),
            dma((2 + 2 * groups,)),
            dma(g_sems), dma(g_sems), dma((n - 1,)), dma((n - 1,)),
            dma((groups, Z + 1)), dma((groups, Z + 1)), dma(g_sems), dma(g_sems),
            dma((n * m - 1,)), dma((n * m - 1,)),
        ],
        compiler_params=pltpu.CompilerParams(
            collective_id=0, has_side_effects=True, vmem_limit_bytes=BIG
        ),
        name="layer",
    )(text_lengths, kv_loc, text_states, video_query, output_grad)
    overall = jnp.sum(parts[:, 0, 0])
    spread = jnp.sqrt(overall / (2.0 * depth * all_features) + 1e-06)
    factor = 1.0 / jnp.maximum(spread, 1.0)
    return attended, query_grad, raw[0] * factor, raw[1] * factor


def solution(mesh):
    n, m = mesh.shape["seq"], mesh.shape["tp"]
    in_specs = (
        P(None, "seq", "tp"),
        P(None, "seq", None),
        P(None, "tp"),
        P(None, "tp"),
        P(),
        P(None, "seq", "tp"),
    )
    out_specs = (P(None, "seq", "tp"), P(None, "seq", "tp"), P("seq", "tp"), P("seq", "tp"))

    def step(*args):
        body = functools.partial(per_device, n, m, args[0].shape[2])
        return jax.shard_map(
            body, mesh=mesh, in_specs=in_specs, out_specs=out_specs, check_vma=False
        )(*args)

    return step
```

```python
import functools
import math

import jax
import jax.numpy as jnp
from jax import lax
from jax.experimental import pallas as pl
from jax.experimental.pallas import tpu as pltpu
from jax.sharding import PartitionSpec as P

HEAD = 128
MESH = pl.DeviceIdType.MESH
NEG = -1e30


def rem(a, b):
    return lax.rem(a, b)


class Place:
    def __init__(self, n):
        self.C = 2
        self.Y = 2
        self.Z = n // 4
        self.n = n
        me = lax.axis_index("seq")
        self.me = me
        self.tp = lax.axis_index("tp")
        self.c = rem(me, 2)
        self.y = rem(me // 2, 2)
        self.z = me // 4

    def dev(self, z, y, c):
        return ((z * self.Y + y) * self.C + c, self.tp)

    def core_peer(self):
        return self.dev(self.z, self.y, 1 - self.c)

    def y_peer(self):
        return self.dev(self.z, 1 - self.y, self.c)

    def z_ahead(self, d):
        return rem(self.z + d, self.Z)

    def z_behind(self, d):
        return rem(self.z + self.Z - d, self.Z)

    def z_peer(self, d):
        return self.dev(self.z_ahead(d), self.y, self.c)


def rcopy(src, dst, ssem, rsem, dev):
    return pltpu.make_async_remote_copy(
        src_ref=src, dst_ref=dst, send_sem=ssem, recv_sem=rsem, device_id=dev, device_id_type=MESH
    )


def greet(devices):
    barrier = pltpu.get_barrier_semaphore()
    for d in devices:
        pl.semaphore_signal(barrier, inc=1, device_id=d, device_id_type=MESH)
    pl.semaphore_wait(barrier, len(devices))


class Gather:
    def __init__(self, pos, block, own, ss, rs):
        self.pos, self.block, self.own, self.ss, self.rs = pos, block, own, ss, rs
        self.sent = []

    def copy(self, src, z, y, c, k, dev):
        d = rcopy(src, self.block(z, y, c), self.ss(k), self.rs(k), dev)
        return d

    def go(self, src, z, y, c, k, dev):
        d = self.copy(src, z, y, c, k, dev)
        d.start()
        self.sent.append(d)

    def start(self):
        p = self.pos
        for d in range(p.Z - 1, 0, -1):
            self.go(self.own, p.z, p.y, p.c, d - 1, p.z_peer(d))
        self.go(self.own, p.z, p.y, p.c, p.Z - 1, p.y_peer())
        self.go(self.own, p.z, p.y, p.c, 2 * p.Z - 1, p.core_peer())

    def arrive_z(self, d):
        p = self.pos
        self.sent[p.Z - 1 - d].wait_recv()
        zz = p.z_behind(d)
        self.go(self.block(zz, p.y, p.c), zz, p.y, p.c, p.Z - 1 + d, p.y_peer())
        self.go(self.block(zz, p.y, p.c), zz, p.y, p.c, 2 * p.Z - 1 + d, p.core_peer())

    def arrive_y(self, d):
        p = self.pos
        zz = p.z_behind(d)
        src = self.block(zz, 1 - p.y, p.c)
        rcopy(src, src, self.ss(p.Z - 1 + d), self.rs(p.Z - 1 + d), p.y_peer()).wait_recv()
        self.go(src, zz, 1 - p.y, p.c, 3 * p.Z - 1 + d, p.core_peer())

    def arrive_core(self):
        p = self.pos
        for d in range(2 * p.Z):
            k = 2 * p.Z - 1 + d
            src = self.own
            rcopy(src, src, self.ss(k), self.rs(k), p.core_peer()).wait_recv()

    def drain(self):
        for d in self.sent:
            d.wait_send()


def flat_rows(x):
    e = x.shape[-1]
    if x.shape[-2] % 16 == 0:
        return x.reshape(-1, e)
    return x.astype(jnp.float32).reshape(-1, e).astype(x.dtype)


def attend(scaling, length, q, g, k, v):
    f32, low = jnp.float32, jnp.bfloat16
    last = (((1,), (1,)), ((), ()))
    head = (((0,), (0,)), ((), ()))
    s = lax.dot_general(k, q, last, preferred_element_type=f32)
    dp = lax.dot_general(v, g, last, preferred_element_type=f32)
    row = lax.broadcasted_iota(jnp.int32, s.shape, 0)
    s = jnp.where(row < length, s, NEG)
    top = jnp.max(s, axis=0, keepdims=True)
    w = jnp.exp2((s - top) * (scaling * math.log2(math.e)))
    inv = 1.0 / jnp.sum(w, axis=0, keepdims=True)
    probs = w * inv
    probs_low = probs.astype(low)
    delta = jnp.sum(probs * dp, axis=0, keepdims=True)
    ds = (probs * (dp - delta) * scaling).astype(low)
    attended = lax.dot_general(v, probs_low, head, preferred_element_type=f32).astype(low).T
    query_grad = lax.dot_general(k, ds, head, preferred_element_type=f32).astype(low).T
    key_grad = jnp.dot(ds, q, preferred_element_type=f32)
    value_grad = jnp.dot(probs_low, g, preferred_element_type=f32)
    return attended, query_grad, key_grad, value_grad


def layer_kernel(n, m, groups, scaling, count, lengths, kv_loc, text, q_hbm, g_hbm, a_hbm, qg_hbm, raw, factor, parts,
                 q, g, a, qg, kv, grads, s1, r1, s2, r2, r3, own, total, cols, cols_t, mine,
                 local, ks, kr, ts, tr, ss, rs, gs, gr, ps, pr):
    f32, low = jnp.float32, jnp.bfloat16
    p = Place(n)
    Z, Y, C = p.Z, p.Y, p.C
    samples, _, features = q.shape
    r = text.shape[1]
    width = cols.shape[-1]
    wide = features // groups
    heads = wide // HEAD
    part = [pl.ds(i * wide, wide) for i in range(groups)]
    loads = [
        pltpu.make_async_copy(q_hbm, q, local.at[0]),
        pltpu.make_async_copy(g_hbm, g, local.at[1]),
    ]
    for cp in loads:
        cp.start()
    flat = p.me * m + p.tp
    peers = []
    for d in range(1, n * m):
        to = rem(flat + d, n * m)
        peers.append((to // m, rem(to, m)))
    greet(peers)

    inward = []
    for i, w in enumerate(part):
        f = Gather(
            p,
            lambda z, y, c, w=w: kv.at[z, y, c, :, :, :, w],
            kv_loc.at[:, :, :, w],
            lambda k, i=i: ks.at[i, k],
            lambda k, i=i: kr.at[i, k],
        )
        f.start()
        inward.append(f)
    direct = []
    for d in range(1, n):
        to = rem(p.me + d, n)
        start = pl.multiple_of(to * width, 128)
        cp = rcopy(
            text.at[:, :, pl.ds(start, width)], cols.at[p.me], ts.at[d - 1], tr.at[d - 1], (to, p.tp)
        )
        cp.start()
        direct.append(cp)
    kv[p.z, p.y, p.c] = kv_loc[...]
    cols[p.me] = text[:, :, pl.ds(pl.multiple_of(p.me * width, 128), width)]

    def in_z(i):
        for d in range(1, Z):
            inward[i].arrive_z(d)

    def in_y(i):
        for d in range(Z):
            inward[i].arrive_y(d)

    def unit(i, b):
        length = lengths[b]

        def one(h, carry):
            w = pl.ds(pl.multiple_of((i * heads + h) * HEAD, HEAD), HEAD)
            k = flat_rows(kv[:, :, :, 0, b, :, w])
            v = flat_rows(kv[:, :, :, 1, b, :, w])
            att, q_grad, k_grad, v_grad = attend(scaling, length, q[b, :, w], g[b, :, w], k, v)
            a[b, :, w] = att
            qg[b, :, w] = q_grad
            grads[:, :, :, 0, b, :, w] = k_grad.reshape(Z, Y, C, r, HEAD).astype(low)
            grads[:, :, :, 1, b, :, w] = v_grad.reshape(Z, Y, C, r, HEAD).astype(low)
            return carry

        lax.fori_loop(0, heads, one, 0)

    sends, stores, outward = [], [], {}
    hold = {}

    def core_send(i):
        w = part[i]
        cp = rcopy(
            grads.at[:, :, 1 - p.c, :, :, :, w], r1.at[:, :, :, :, :, w], ss.at[i, 0], rs.at[i, 0],
            p.core_peer(),
        )
        cp.start()
        sends.append(cp)
        hold[i, 0] = cp
        for src, dst, k in ((a, a_hbm, 0), (qg, qg_hbm, 1)):
            st = pltpu.make_async_copy(src.at[:, :, w], dst.at[:, :, w], local.at[2 + 2 * i + k])
            st.start()
            stores.append(st)

    def core_sum(i):
        w = part[i]
        hold[i, 0].wait_recv()
        for far in (True, False):
            yy = 1 - p.y if far else p.y
            s1[:, yy, :, :, :, w] = (
                grads[:, yy, p.c, :, :, :, w].astype(f32) + r1[:, yy, :, :, :, w].astype(f32)
            ).astype(low)
            if far:
                cp = rcopy(
                    s1.at[:, yy, :, :, :, w], r2.at[:, :, :, :, w], ss.at[i, 1], rs.at[i, 1], p.y_peer()
                )
                cp.start()
                sends.append(cp)
                hold[i, 1] = cp

    def y_sum(i):
        w = part[i]
        hold[i, 1].wait_recv()
        for d in range(Z - 1, 0, -1):
            zz = p.z_ahead(d)
            s2[zz, :, :, :, w] = (
                s1[zz, p.y, :, :, :, w].astype(f32) + r2[zz, :, :, :, w].astype(f32)
            ).astype(low)
            cp = rcopy(
                s2.at[zz, :, :, :, w], r3.at[d - 1, :, :, :, w], ss.at[i, 1 + d], rs.at[i, 1 + d],
                p.z_peer(d),
            )
            cp.start()
            sends.append(cp)
            hold[i, 1 + d] = cp

    def z_sum(i):
        w = part[i]
        x = s1[p.z, p.y, :, :, :, w].astype(f32) + r2[p.z, :, :, :, w].astype(f32)
        for d in range(1, Z):
            hold[i, 1 + d].wait_recv()
            x = x + r3[d - 1, :, :, :, w].astype(f32)
        own[:, :, :, w] = x.astype(low)
        f = Gather(
            p,
            lambda z, y, c: total.at[z, y, c, :, :, :, w],
            own.at[:, :, :, w],
            lambda k: gs.at[i, k],
            lambda k: gr.at[i, k],
        )
        f.start()
        total[p.z, p.y, p.c, :, :, :, w] = x.astype(low)
        outward[i] = f

    def out_z(i):
        for d in range(1, Z):
            outward[i].arrive_z(d)

    def out_y(i):
        for d in range(Z):
            outward[i].arrive_y(d)

    squares = []

    def out_core(i):
        if i == 0:
            for cp in direct:
                cp.wait_recv()
            cols_t[...] = flat_rows(cols[...]).T
        outward[i].arrive_core()
        for kind in range(2):
            x = flat_rows(total[:, :, :, kind, :, :, part[i]])
            y = jnp.dot(cols_t[...], x, preferred_element_type=f32)
            raw[kind, :, part[i]] = y
            squares.append(jnp.sum((y * y).reshape(-1, 8, wide), axis=0))

    stages = (core_sum, y_sum, z_sum, out_z, out_y, out_core)
    pending = {}

    def turn():
        for i in sorted(pending):
            stages[pending[i]](i)
            pending[i] += 1
            if pending[i] == len(stages):
                del pending[i]

    in_z(0)
    in_y(0)
    if groups > 1:
        in_z(1)
    inward[0].arrive_core()
    for cp in loads:
        cp.wait()
    for i in range(groups):
        for b in range(samples):
            unit(i, b)
            if b == 0:
                if i + 1 < groups:
                    in_y(i + 1)
                if i + 2 < groups:
                    in_z(i + 2)
                turn()
        core_send(i)
        if i + 1 < groups:
            inward[i + 1].arrive_core()
        turn()
        pending[i] = 0
    while pending:
        turn()
    acc = squares[0]
    for x in squares[1:]:
        acc = acc + x
    mine[...] = jnp.broadcast_to(jnp.sum(acc, keepdims=True), mine.shape)
    last = []
    for d, dev in enumerate(peers):
        cp = rcopy(mine, parts.at[flat], ps.at[d], pr.at[d], dev)
        cp.start()
        last.append(cp)
    parts[flat] = mine[...]
    for st in stores:
        st.wait()
    for f in inward:
        f.drain()
    for i in sorted(outward):
        outward[i].drain()
    for cp in direct + sends:
        cp.wait_send()
    for cp in last:
        cp.wait()
    spread = jnp.sqrt(jnp.sum(parts[...], axis=0) / count + 1e-06)
    factor[...] = 1.0 / jnp.maximum(spread, 1.0)


VM = pl.BlockSpec(memory_space=pltpu.VMEM)
ANY = pl.BlockSpec(memory_space=pl.ANY)
BIG = 40 * 1024 * 1024


def per_device(n, m, all_features, video_query, text_states, key_weight, value_weight, text_lengths, output_grad):
    samples, rows, features = video_query.shape
    _, r, depth = text_states.shape
    heads = features // HEAD
    groups = 4 if heads % 4 == 0 else (3 if heads % 3 == 0 else 1)
    low, f32 = jnp.bfloat16, jnp.float32
    Z, Y, C = n // 4, 2, 2
    dma, vmem = pltpu.SemaphoreType.DMA, pltpu.VMEM
    k_loc = jnp.dot(text_states, key_weight, preferred_element_type=f32).astype(low)
    v_loc = jnp.dot(text_states, value_weight, preferred_element_type=f32).astype(low)
    kv_loc = jnp.stack((k_loc, v_loc))
    block = (2, samples, r, features)
    full = vmem((Z, Y, C) + block, low)
    half = vmem((Z, Y) + block, low)
    quarter = vmem((Z,) + block, low)
    video = vmem(video_query.shape, low)
    video_out = jax.ShapeDtypeStruct(video_query.shape, low)
    g_sems = (groups, 4 * Z - 1)
    count = 2.0 * depth * all_features
    attended, query_grad, raw, factor = pl.pallas_call(
        functools.partial(layer_kernel, n, m, groups, 1.0 / math.sqrt(HEAD), count),
        out_shape=(
            video_out,
            video_out,
            jax.ShapeDtypeStruct((2, depth // n, features), f32),
            jax.ShapeDtypeStruct((8, 128), f32),
        ),
        in_specs=[pl.BlockSpec(memory_space=pltpu.SMEM), VM, VM, ANY, ANY],
        out_specs=(ANY, ANY, VM, VM),
        scratch_shapes=[
            vmem((n * m, 8, 128), f32),
            video, video, video, video,
            full, full, half, half, quarter, quarter, vmem((Z - 1,) + block, low), vmem(block, low), full,
            vmem((n, samples, r, depth // n), low), vmem((depth // n, n * samples * r), low),
            vmem((8, 128), f32),
            dma((2 + 2 * groups,)),
            dma(g_sems), dma(g_sems), dma((n - 1,)), dma((n - 1,)),
            dma((groups, Z + 1)), dma((groups, Z + 1)), dma(g_sems), dma(g_sems),
            dma((n * m - 1,)), dma((n * m - 1,)),
        ],
        compiler_params=pltpu.CompilerParams(
            collective_id=0, has_side_effects=True, vmem_limit_bytes=BIG
        ),
        name="layer",
    )(text_lengths, kv_loc, text_states, video_query, output_grad)
    factor = factor[0, 0]
    return attended, query_grad, raw[0] * factor, raw[1] * factor


def solution(mesh):
    n, m = mesh.shape["seq"], mesh.shape["tp"]
    in_specs = (
        P(None, "seq", "tp"),
        P(None, "seq", None),
        P(None, "tp"),
        P(None, "tp"),
        P(),
        P(None, "seq", "tp"),
    )
    out_specs = (P(None, "seq", "tp"), P(None, "seq", "tp"), P("seq", "tp"), P("seq", "tp"))

    def step(*args):
        body = functools.partial(per_device, n, m, args[0].shape[2])
        return jax.shard_map(
            body, mesh=mesh, in_specs=in_specs, out_specs=out_specs, check_vma=False
        )(*args)

    return step
```
